32 devices in a mesh: rep: 2 (over x), seq: 8 (over z, y), tp: 2 (over core).
Axes of the slice: x: 2, y: 2, z: 4, core: 2. Of those that a mesh axis runs over, the one named last changes fastest.
Arguments:
- prefill_query: bfloat16 [8192, 2048], P(('rep', 'seq'), 'tp'), parts along dimension 0, may hold values from -50 to 50
- prefill_key: bfloat16 [8192, 512], P(('rep', 'seq'), 'tp'), parts along dimension 0, may hold values from -6 to 6
- prefill_value: bfloat16 [8192, 512], P(('rep', 'seq'), 'tp'), parts along dimension 0, may hold values from -6 to 6
- doc_ids: int32 [8192], P('rep'), parts along dimension 0, may hold values from 0 to 3, never falling along the last dimension, each value on 1 to 2048 neighbouring positions
- head_window: int32 [16], P('tp'), may hold values from 1024 to 4096, as said below
- dec_query: bfloat16 [128, 2048], P('rep', 'tp'), parts along dimension 0, may hold values from -50 to 50
- dec_key: bfloat16 [128, 512], P('rep', 'tp'), parts along dimension 0, may hold values from -6 to 6
- dec_value: bfloat16 [128, 512], P('rep', 'tp'), parts along dimension 0, may hold values from -6 to 6
- cache_key: bfloat16 [65536, 512], P(('rep', 'seq'), 'tp'), parts along dimension 0, may hold values from -6 to 6
- cache_value: bfloat16 [65536, 512], P(('rep', 'seq'), 'tp'), parts along dimension 0, may hold values from -6 to 6
- page_order: int32 [512], P(('rep', 'seq')), parts along dimension 0, may hold values from 0 to 255, each once
- lengths: int32 [128], P('rep'), parts along dimension 0, may hold values from 1 to 512, 16384 in all
- out_proj: bfloat16 [2048, 4096], P('tp'), may hold values from -0.125 to 0.125
Outputs:
- prompt_out: bfloat16 [8192, 4096], P(('rep', 'seq', 'tp')), parts along dimension 0
- decode_out: bfloat16 [128, 4096], P(('rep', 'tp')), parts along dimension 0
The draws below stay inside these ranges and needn't reach their ends.
There are 2 independent parts, one for each index of `rep`. The reference program is written for one: setup_inputs(seed, part) draws one part's arguments, and reference() takes and returns one part's arrays. A program takes and returns all parts, laid end to end along the dimension named above; an argument that names none is the same for every part. Nothing has to cross between parts.
Inputs may be any that keep to these rules, and one draw needn't show every extreme that they name: `head_window`: some head has window 4096.
All inputs are finite; a program needn't handle non-finite values.
Results may differ from the reference program's by a relative error of at most 0.015.
Values may be sent and summed in bfloat16 or wider, within the bound.
A program may use at most 256 MiB of HBM per device.

```python
import math
import jax
import jax.numpy as jnp
import numpy as np
from jax import lax

D = 4096
HD = 128
HEADS = 16
KV_HEADS = 4
WINDOW = 4096
REQS = 64
PAGE = 128
TOKENS = 4096
PAGES = 256
MAXLEN = 512
N_TP = 2


def prompt_keys(key):
    base = jax.random.fold_in(key, 7)
    keys = jnp.clip(jax.random.normal(base, (TOKENS, KV_HEADS * HD), jnp.float32), -6.0, 6.0)
    return keys


def draw_prefill_key(key, part):
    return prompt_keys(key).astype(jnp.bfloat16)


def draw_prefill_query(key, part):
    base = jax.random.fold_in(key, 8)
    queries = jnp.clip(jax.random.normal(base, (TOKENS, HEADS * HD), jnp.float32), -6.0, 6.0)
    return queries.astype(jnp.bfloat16)


def decode_keys(key):
    base = jax.random.fold_in(key, 9)
    keys = jnp.clip(jax.random.normal(base, (REQS, KV_HEADS * HD), jnp.float32), -6.0, 6.0)
    return keys


def draw_dec_key(key, part):
    return decode_keys(key).astype(jnp.bfloat16)


def draw_dec_query(key, part):
    base = jax.random.fold_in(key, 10)
    queries = jnp.clip(jax.random.normal(base, (REQS, HEADS * HD), jnp.float32), -6.0, 6.0)
    return queries.astype(jnp.bfloat16)


def draw_head_window(key, part):
    widths = jax.random.randint(jax.random.fold_in(key, 3), (HEADS,), WINDOW // 4, WINDOW + 1)
    picked = jax.random.randint(jax.random.fold_in(key, 4), (), 0, HEADS)
    return jnp.where(jnp.arange(HEADS) == picked, WINDOW, widths).astype(jnp.int32)


def shard_levels(key, shape, split, least, largest):
    factor_of, own = 1.0, jax.random.fold_in(key, 6)
    for dim, parts in split:
        draws = jnp.exp(jax.random.uniform(jax.random.fold_in(own, dim), (parts,), jnp.float32, least / len(split), largest / len(split)))
        factor_of = factor_of * jnp.repeat(draws, shape[dim] // parts).reshape([-1 if axis == dim else 1 for axis in range(len(shape))])
    return factor_of


def length_profile(count, total, most, skew):
    weights = [(1 << 20) // math.isqrt(grade ** skew) + 1 for grade in range(2, count + 1)]
    spare, holding = total - most - (count - 1), [1] * (count - 1)
    while spare > 0:
        free = [i for i in range(count - 1) if holding[i] < most]
        mass, budget = sum([weights[i] for i in free]), spare
        for i in free:
            extra = min(most - holding[i], max(1, budget * weights[i] // mass), spare)
            holding[i] = holding[i] + extra
            spare = spare - extra
    return np.array([most] + holding)


def uneven(stream_key, count, total, bound, lean):
    if count == 2:
        one = jax.random.randint(stream_key, (), max(1, total - bound), min(bound, total - 1) + 1)
        return jnp.stack([one, total - one])
    tallies = jnp.asarray(length_profile(count, total, bound, lean), jnp.int32)
    pairs = (count - 1) // 2
    source_of, taker = tallies[1:1 + 2 * pairs:2], tallies[2:2 + 2 * pairs:2]
    margin = jnp.minimum(source_of - 1, bound - taker)
    passed = jax.random.randint(jax.random.fold_in(stream_key, 1), (pairs,), 0, 1 << 20) % (margin + 1)
    tallies = tallies.at[1:1 + 2 * pairs:2].set(source_of - passed).at[2:2 + 2 * pairs:2].set(taker + passed)
    return tallies[jax.random.permutation(jax.random.fold_in(stream_key, 2), count)]


def normal_values(key, extent, scale, bound, pieces=(), kind=jnp.bfloat16):
    level = shard_levels(key, extent, pieces, -0.22, 0.18) if pieces else 1.0
    entries = jax.random.normal(key, extent, jnp.float32) * scale * level
    return jnp.minimum(jnp.maximum(entries, -bound), bound).astype(kind)


def setup_inputs(seed: int = 0, part: int = 0) -> dict:
    streams_of = jax.random.split(jax.random.key(seed), 14)
    part_keys = jax.random.split(jax.random.fold_in(streams_of[13], part), 14)
    return {
        "prefill_query": draw_prefill_query(jax.random.fold_in(jax.random.fold_in(streams_of[13], part), 71), part),
        "prefill_key": draw_prefill_key(jax.random.fold_in(jax.random.fold_in(streams_of[13], part), 71), part),
        "prefill_value": normal_values(part_keys[2], (TOKENS, KV_HEADS * HD), 1.0, 6.0, ((0, 8), (1, 2))),
        "doc_ids": jnp.searchsorted(jnp.cumsum(uneven(part_keys[3], 4, TOKENS, TOKENS // 2, 1)), jnp.arange(TOKENS), side="right").astype(jnp.int32),
        "head_window": draw_head_window(jax.random.fold_in(streams_of[13], 71), part),
        "dec_query": draw_dec_query(jax.random.fold_in(jax.random.fold_in(streams_of[13], part), 71), part),
        "dec_key": draw_dec_key(jax.random.fold_in(jax.random.fold_in(streams_of[13], part), 71), part),
        "dec_value": normal_values(part_keys[7], (REQS, KV_HEADS * HD), 1.0, 6.0, ((1, 2),)),
        "cache_key": normal_values(part_keys[8], (PAGES * PAGE, KV_HEADS * HD), 1.0, 6.0, ((0, 8), (1, 2))),
        "cache_value": normal_values(part_keys[9], (PAGES * PAGE, KV_HEADS * HD), 1.0, 6.0, ((0, 8), (1, 2))),
        "page_order": jax.random.permutation(part_keys[10], PAGES).astype(jnp.int32),
        "lengths": uneven(part_keys[11], REQS, REQS * MAXLEN // 2, MAXLEN, 2).astype(jnp.int32),
        "out_proj": normal_values(streams_of[12], (HEADS * HD, D), (HEADS * HD) ** -0.5, 0.125, ((0, 2),)),
    }


masked_score = -1e+30

def round_half(values):
    return lax.optimization_barrier(values.astype(jnp.bfloat16)).astype(jnp.float32)

def project(rows_matrix, out_proj):
    columns = HEADS * HD // N_TP
    total = jnp.zeros((rows_matrix.shape[0], D), jnp.float32)
    for group in range(N_TP):
        partial_sum = jnp.dot(rows_matrix[:, group * columns:(group + 1) * columns], out_proj[group * columns:(group + 1) * columns], preferred_element_type=jnp.float32)
        total = total + round_half(partial_sum)
    return total.astype(jnp.bfloat16)

def reference(prefill_query, prefill_key, prefill_value, doc_ids, head_window, dec_query, dec_key, dec_value, cache_key, cache_value, page_order, lengths, out_proj):
    group_size = HEADS // KV_HEADS
    scale_factor = 1.0 / math.sqrt(HD)
    block = math.gcd(512, TOKENS)
    key_pad = jnp.pad(prefill_key, ((WINDOW, 0), (0, 0)))
    value_pad = jnp.pad(prefill_value, ((WINDOW, 0), (0, 0)))
    doc_pad = jnp.pad(doc_ids, (WINDOW, 0), constant_values=-1)
    windows = head_window.reshape(KV_HEADS, group_size)

    def one_block(index):
        start = (index * block).astype(jnp.int32)
        queries = lax.dynamic_slice_in_dim(prefill_query, start, block, 0).reshape(block, KV_HEADS, group_size, HD).astype(jnp.float32)
        keys = lax.dynamic_slice_in_dim(key_pad, start, block + WINDOW, 0).reshape(block + WINDOW, KV_HEADS, HD).astype(jnp.float32)
        values = lax.dynamic_slice_in_dim(value_pad, start, block + WINDOW, 0).reshape(block + WINDOW, KV_HEADS, HD).astype(jnp.float32)
        query_doc = lax.dynamic_slice_in_dim(doc_ids, start, block, 0)
        key_doc = lax.dynamic_slice_in_dim(doc_pad, start, block + WINDOW, 0)
        query_pos = start + jnp.arange(block, dtype=jnp.int32)
        key_pos = start - WINDOW + jnp.arange(block + WINDOW, dtype=jnp.int32)
        gap = query_pos[:, None] - key_pos[None, :]
        allowed = (gap >= 0) & (query_doc[:, None] == key_doc[None, :])
        allowed = allowed[None, None] & (gap[None, None] < windows[:, :, None, None])
        scores = jnp.einsum('tkgd,skd->kgts', queries, keys) * scale_factor
        scores = jnp.where(allowed, scores, masked_score)
        highest = lax.optimization_barrier(jnp.max(scores, axis=-1))
        weights = jnp.where(allowed, jnp.exp(scores - highest[..., None]), 0.0)
        totals = lax.optimization_barrier(jnp.sum(weights, axis=-1))
        output = jnp.einsum('kgts,skd->kgtd', round_half(weights), values) / totals[..., None]
        return output.transpose(2, 0, 1, 3).reshape(block, HEADS * HD).astype(jnp.bfloat16)
    prompt_attn = lax.map(one_block, jnp.arange(TOKENS // block, dtype=jnp.int32)).reshape(TOKENS, HEADS * HD)
    prompt_out = project(prompt_attn, out_proj)
    inverse = jnp.zeros((PAGES,), jnp.int32).at[page_order].set(jnp.arange(PAGES, dtype=jnp.int32))
    cached_keys = cache_key.reshape(PAGES, PAGE, KV_HEADS * HD)[inverse].reshape(REQS, MAXLEN, KV_HEADS, HD).astype(jnp.float32)
    cached_values = cache_value.reshape(PAGES, PAGE, KV_HEADS * HD)[inverse].reshape(REQS, MAXLEN, KV_HEADS, HD).astype(jnp.float32)
    queries = dec_query.reshape(REQS, KV_HEADS, group_size, HD).astype(jnp.float32)
    own_keys = dec_key.reshape(REQS, KV_HEADS, HD).astype(jnp.float32)
    own_values = dec_value.reshape(REQS, KV_HEADS, HD).astype(jnp.float32)
    scores = jnp.einsum('rkgd,rskd->rkgs', queries, cached_keys) * scale_factor
    valid = (jnp.arange(MAXLEN, dtype=jnp.int32)[None, :] < lengths[:, None])[:, None, None, :]
    scores = jnp.where(valid, scores, masked_score)
    own_scores = jnp.einsum('rkgd,rkd->rkg', queries, own_keys) * scale_factor
    highest = jnp.maximum(lax.optimization_barrier(jnp.max(scores, axis=-1)), own_scores)
    weights = jnp.where(valid, jnp.exp(scores - highest[..., None]), 0.0)
    own_weights = jnp.exp(own_scores - highest)
    totals = lax.optimization_barrier(jnp.sum(weights, axis=-1)) + own_weights
    output = jnp.einsum('rkgs,rskd->rkgd', round_half(weights), cached_values) + round_half(own_weights)[..., None] * own_values[:, :, None, :]
    decode_attn = (output / totals[..., None]).reshape(REQS, HEADS * HD).astype(jnp.bfloat16)
    decode_out = project(decode_attn, out_proj)
    return (prompt_out, decode_out)
```

```python
import functools
import math

import jax
import jax.numpy as jnp
from jax import lax
from jax.experimental import pallas as pl
from jax.experimental.pallas import tpu as pltpu
from jax.sharding import PartitionSpec as P

HD = 128
WINDOW = 4096
PAGE = 128
MASKED = -1e30
FLOOR = -1e29
MESH = pl.DeviceIdType.MESH


def dot_t(a, b):
    return lax.dot_general(a, b, (((1,), (1,)), ((), ())), preferred_element_type=jnp.float32)


def wide(column, width):
    return jnp.concatenate([column] * (width // column.shape[1]), axis=1)


def kernel(
    n, back, q, k, v, lo, col_req, dq, dk, dv, ck, cv, w,
    out_p, out_d,
    kv, top, tot, acc, rows, ckv, cvv, wv, part, gathered, mine, att, outgoing, incoming,
    local_sem, zs, zr, ys, yr, ps, pr, fs, fr, ts, tr,
):
    me = lax.axis_index("seq")
    core = lax.axis_index("tp")
    other = 1 - core
    odd = lax.rem(me, 2)
    partner = me + 1 - 2 * odd
    tokens = q.shape[0]
    heads = q.shape[1] // HD
    groups = k.shape[1] // HD
    per = heads // groups
    reqs = dq.shape[0]
    scale = 1.0 / math.sqrt(HD)
    exp_scale = scale * math.log2(math.e)

    loads = [
        pltpu.make_async_copy(ck, ckv, local_sem.at[0]),
        pltpu.make_async_copy(cv, cvv, local_sem.at[1]),
        pltpu.make_async_copy(w, wv, local_sem.at[2]),
    ]
    for load in loads:
        load.start()

    barrier = pltpu.get_barrier_semaphore()

    def greet(d, carry):
        pl.semaphore_signal(
            barrier, inc=1, device_id={"seq": lax.rem(me + d, n)}, device_id_type=MESH
        )
        return carry

    lax.fori_loop(1, n, greet, 0)
    pl.semaphore_signal(barrier, inc=1, device_id={"tp": other}, device_id_type=MESH)
    pl.semaphore_wait(barrier, n)

    def source(s, g, i):
        if s == 0:
            return (k, v)[i].at[:, pl.ds(g * HD, HD)]
        return kv.at[s - 1, g, i]

    def along(s, g, i):
        return pltpu.make_async_remote_copy(
            src_ref=source(s, g, i),
            dst_ref=kv.at[s + 1, g, i],
            send_sem=zs.at[s // 2, g, i],
            recv_sem=zr.at[s // 2, g, i],
            device_id={"seq": lax.rem(me + 2, n)},
            device_id_type=MESH,
        )

    def across(s, h, g, i):
        return pltpu.make_async_remote_copy(
            src_ref=source(s, g, i),
            dst_ref=kv.at[2 * h - 2, g, i],
            send_sem=ys.at[h - 1, g, i],
            recv_sem=yr.at[h - 1, g, i],
            device_id={"seq": partner},
            device_id_type=MESH,
        )

    def forward(s, g, finish=False):
        act = (lambda c: c.wait_send()) if finish else (lambda c: c.start())
        if s + 2 <= back:
            @pl.when((me >= s) & (me + 2 < n))
            def _():
                for i in range(2):
                    act(along(s, g, i))

            @pl.when((me >= s) & (odd == 0))
            def _():
                for i in range(2):
                    act(across(s, s // 2 + 1, g, i))
        if s >= 2:
            @pl.when((me >= s) & (odd == 1))
            def _():
                for i in range(2):
                    act(across(s, s // 2, g, i))

    def arrive(s, g):
        @pl.when(me >= s)
        def _():
            for i in range(2):
                if s % 2 == 0:
                    along(s - 2, g, i).wait_recv()
                else:
                    across(s + 1, (s + 1) // 2, g, i).wait_recv()

        if s % 2 == 0:
            forward(s, g)

    def attend(s, g):
        def one_head(r, carry):
            head = g * per + r
            queries = q[:, pl.ds(pl.multiple_of(head * HD, HD), HD)]
            if s == 0:
                keys = k[:, g * HD:(g + 1) * HD]
                values = v[:, g * HD:(g + 1) * HD]
            else:
                keys = kv[s - 1, g, 0]
                values = kv[s - 1, g, 1]
            scores = dot_t(queries, keys)
            column = lax.broadcasted_iota(jnp.int32, (tokens, tokens), 1)
            limit = lo[head] - (me - s) * tokens
            allowed = column >= limit
            if s == 0:
                allowed = allowed & (
                    column <= lax.broadcasted_iota(jnp.int32, (tokens, tokens), 0)
                )
            scores = jnp.where(allowed, scores, MASKED)
            high = jnp.max(scores, axis=1, keepdims=True) * exp_scale
            high = jnp.broadcast_to(high, (tokens, HD))
            if s > 0:
                old = top[head]
                high = jnp.maximum(high, old)
            weights = jnp.exp2(scores * exp_scale - wide(high, tokens))
            total = jnp.broadcast_to(jnp.sum(weights, axis=1, keepdims=True), (tokens, HD))
            added = jnp.dot(
                weights.astype(jnp.bfloat16), values, preferred_element_type=jnp.float32
            )
            if s > 0:
                shrink = jnp.exp2(old - high)
                total = total + tot[head] * shrink
                added = added + acc[head] * shrink
            top[head] = high
            tot[head] = total
            acc[head] = added
            return carry

        @pl.when(me >= s)
        def _():
            lax.fori_loop(0, per, one_head, 0)

    def to_owner(head):
        return pltpu.make_async_remote_copy(
            src_ref=part.at[head],
            dst_ref=gathered.at[me],
            send_sem=ps.at[head],
            recv_sem=pr.at[me],
            device_id={"seq": head},
            device_id_type=MESH,
        )

    def decode_partials():
        loads[0].wait()
        loads[1].wait()
        pages = col_req.shape[0]
        step = math.gcd(pages, 8)
        row_req = lax.rem(
            lax.broadcasted_iota(jnp.int32, (per * reqs, step * PAGE), 0), reqs
        )
        for g in range(groups):
            queries = jnp.concatenate(
                [dq[:, (g * per + r) * HD:(g * per + r + 1) * HD] for r in range(per)], axis=0
            )

            def block(b, carry):
                high_old, total_old, acc_old = carry
                span = pl.ds(pl.multiple_of(b * step * PAGE, step * PAGE), step * PAGE)
                keys = ckv[span, g * HD:(g + 1) * HD]
                values = cvv[span, g * HD:(g + 1) * HD]
                reqs_of = col_req[pl.ds(pl.multiple_of(b * step, step), step), :]
                reqs_of = jnp.concatenate([reqs_of[i:i + 1, :] for i in range(step)], axis=1)
                scores = jnp.where(row_req == reqs_of, dot_t(queries, keys), MASKED)
                high = jnp.max(scores, axis=1, keepdims=True)
                high = jnp.maximum(high, FLOOR) * exp_scale
                high = jnp.maximum(jnp.broadcast_to(high, (per * reqs, HD)), high_old)
                weights = jnp.exp2(scores * exp_scale - wide(high, step * PAGE))
                total = jnp.sum(weights, axis=1, keepdims=True)
                shrink = jnp.exp2(high_old - high)
                added = jnp.dot(
                    weights.astype(jnp.bfloat16), values, preferred_element_type=jnp.float32
                )
                return (high, total + total_old * shrink, added + acc_old * shrink)

            zero = jnp.zeros((per * reqs, HD), jnp.float32)
            high, total, added = lax.fori_loop(
                0, pages // step, block, (zero + FLOOR * exp_scale, zero, zero)
            )
            for r in range(per):
                cut = slice(r * reqs, (r + 1) * reqs)
                part[g * per + r, 0] = high[cut]
                part[g * per + r, 1] = total[cut]
                part[g * per + r, 2] = added[cut]
        for head in range(heads):
            @pl.when(me != head)
            def _():
                to_owner(head).start()

    def from_owner(d):
        return pltpu.make_async_remote_copy(
            src_ref=mine,
            dst_ref=att.at[me],
            send_sem=fs.at[d - 1],
            recv_sem=fr.at[me],
            device_id={"seq": lax.rem(me + d, n)},
            device_id_type=MESH,
        )

    def wait_partial(j):
        return pltpu.make_async_remote_copy(
            src_ref=part.at[0],
            dst_ref=gathered.at[j],
            send_sem=ps.at[0],
            recv_sem=pr.at[j],
            device_id={"seq": partner},
            device_id_type=MESH,
        )

    def wait_final(head):
        return pltpu.make_async_remote_copy(
            src_ref=mine,
            dst_ref=att.at[head],
            send_sem=fs.at[0],
            recv_sem=fr.at[head],
            device_id={"seq": partner},
            device_id_type=MESH,
        )

    def decode_merge():
        @pl.when(me < heads)
        def _():
            head = me
            queries = dq[:, pl.ds(pl.multiple_of(head * HD, HD), HD)].astype(jnp.float32)
            group = pl.ds(pl.multiple_of((head // per) * HD, HD), HD)
            own = jnp.sum(queries * dk[:, group].astype(jnp.float32), axis=1, keepdims=True)
            own = jnp.broadcast_to(own * exp_scale, (reqs, HD))
            high = jnp.maximum(own, part[head, 0])
            shrink = jnp.exp2(part[head, 0] - high)
            weight = jnp.exp2(own - high)
            total = weight + part[head, 1] * shrink
            value = dv[:, group].astype(jnp.float32)
            summed = (
                weight.astype(jnp.bfloat16).astype(jnp.float32) * value
                + part[head, 2] * shrink
            )

            def take(d, carry):
                high_old, total_old, sum_old = carry
                j = lax.rem(me + d, n)
                wait_partial(j).wait_recv()
                fresh = jnp.maximum(high_old, gathered[j, 0])
                left = jnp.exp2(high_old - fresh)
                right = jnp.exp2(gathered[j, 0] - fresh)
                return (
                    fresh,
                    total_old * left + gathered[j, 1] * right,
                    sum_old * left + gathered[j, 2] * right,
                )

            high, total, summed = lax.fori_loop(1, n, take, (high, total, summed))
            final = (summed / total).astype(jnp.bfloat16)
            mine[...] = final

            def send(d, carry):
                from_owner(d).start()
                return carry

            lax.fori_loop(1, n, send, 0)

    for g in range(groups):
        forward(0, g)
    for g in range(groups):
        attend(0, g)
    arrive(2, 0)
    decode_partials()
    for g in range(1, groups):
        arrive(2, g)
    for g in range(groups):
        attend(2, g)
    for h in range(1, back // 2 + 1):
        for g in range(groups):
            if 2 * h + 2 <= back:
                arrive(2 * h + 2, g)
            arrive(2 * h - 1, g)
            attend(2 * h - 1, g)
        if h == 1:
            decode_merge()
        if 2 * h + 2 <= back:
            for g in range(groups):
                attend(2 * h + 2, g)

    half = tokens // 2
    half_reqs = reqs // 2
    for head in range(heads):
        cut = slice(head * HD, (head + 1) * HD)
        done = (acc[head] / tot[head]).astype(jnp.bfloat16)
        for c in range(2):
            rows[c, :half, cut] = done[c * half:(c + 1) * half]

        @pl.when(me == head)
        def _():
            for c in range(2):
                rows[c, half:, cut] = mine[c * half_reqs:(c + 1) * half_reqs]

        @pl.when(me != head)
        def _():
            wait_final(head).wait_recv()
            for c in range(2):
                rows[c, half:, cut] = att[head, c * half_reqs:(c + 1) * half_reqs]

    loads[2].wait()
    blocks = outgoing.shape[0]
    width = outgoing.shape[2]

    def exchange(b):
        return pltpu.make_async_remote_copy(
            src_ref=outgoing.at[b],
            dst_ref=incoming.at[b],
            send_sem=ts.at[b],
            recv_sem=tr.at[b],
            device_id={"tp": other},
            device_id_type=MESH,
        )

    def project(c, b):
        span = pl.ds(pl.multiple_of(b * width, width), width)
        return jnp.dot(rows[c], wv[:, span], preferred_element_type=jnp.float32)

    def give(b, carry):
        outgoing[b] = project(other, b).astype(jnp.bfloat16)
        exchange(b).start()
        return carry

    def keep(b, carry):
        own = project(core, b).astype(jnp.bfloat16).astype(jnp.float32)
        exchange(b).wait_recv()
        total = (own + incoming[b].astype(jnp.float32)).astype(jnp.bfloat16)
        span = pl.ds(pl.multiple_of(b * width, width), width)
        out_p[:, span] = total[:half]
        out_d[:, span] = total[half:]
        return carry

    lax.fori_loop(0, blocks, give, 0)
    lax.fori_loop(0, blocks, keep, 0)

    def sent(b, carry):
        exchange(b).wait_send()
        return carry

    lax.fori_loop(0, blocks, sent, 0)
    for s in range(0, back + 1, 2):
        for g in range(groups):
            forward(s, g, finish=True)
    for head in range(heads):
        @pl.when(me != head)
        def _():
            to_owner(head).wait_send()

    @pl.when(me < heads)
    def _():
        def sent_final(d, carry):
            from_owner(d).wait_send()
            return carry

        lax.fori_loop(1, n, sent_final, 0)


def on_device(
    n, prefill_query, prefill_key, prefill_value, doc_ids, head_window, dec_query, dec_key,
    dec_value, cache_key, cache_value, page_order, lengths, out_proj,
):
    tokens, width = prefill_query.shape
    heads = width // HD
    groups = prefill_key.shape[1] // HD
    reqs = dec_query.shape[0]
    model = out_proj.shape[1]
    pages = page_order.shape[0]
    reach = min(doc_ids.shape[0] // 2, WINDOW)
    back = -(-reach // tokens)
    back += back % 2

    my_start = lax.axis_index("seq") * tokens
    query_doc = lax.dynamic_slice_in_dim(doc_ids, my_start, tokens, 0)
    doc_start = jnp.sum((doc_ids[None, :] < query_doc[:, None]).astype(jnp.int32), axis=1)
    position = my_start + jnp.arange(tokens, dtype=jnp.int32)
    lo = jnp.maximum(doc_start[None, :], position[None, :] - head_window[:, None] + 1)[..., None]

    pages_request = pages * n // reqs
    owner = page_order // pages_request
    slot = page_order % pages_request
    member = owner[:, None] == jnp.arange(reqs, dtype=jnp.int32)[None, :]
    length = jnp.sum(jnp.where(member, lengths[None, :], 0), axis=1)
    place = slot[:, None] * PAGE + jnp.arange(PAGE, dtype=jnp.int32)[None, :]
    col_req = jnp.where(place < length[:, None], owner[:, None], -1)

    vmem = pl.BlockSpec(memory_space=pltpu.VMEM)
    hbm = pl.BlockSpec(memory_space=pl.ANY)
    block = 512
    blocks = model // block
    merged = (tokens + reqs) // 2
    dma = pltpu.SemaphoreType.DMA
    return pl.pallas_call(
        functools.partial(kernel, n, back),
        out_shape=(
            jax.ShapeDtypeStruct((tokens // 2, model), jnp.bfloat16),
            jax.ShapeDtypeStruct((reqs // 2, model), jnp.bfloat16),
        ),
        in_specs=[vmem] * 8 + [hbm] * 3,
        out_specs=(vmem, vmem),
        scratch_shapes=[
            pltpu.VMEM((back, groups, 2, tokens, HD), jnp.bfloat16),
            pltpu.VMEM((heads, tokens, HD), jnp.float32),
            pltpu.VMEM((heads, tokens, HD), jnp.float32),
            pltpu.VMEM((heads, tokens, HD), jnp.float32),
            pltpu.VMEM((2, merged, heads * HD), jnp.bfloat16),
            pltpu.VMEM(cache_key.shape, jnp.bfloat16),
            pltpu.VMEM(cache_value.shape, jnp.bfloat16),
            pltpu.VMEM(out_proj.shape, jnp.bfloat16),
            pltpu.VMEM((heads, 3, reqs, HD), jnp.float32),
            pltpu.VMEM((n, 3, reqs, HD), jnp.float32),
            pltpu.VMEM((reqs, HD), jnp.bfloat16),
            pltpu.VMEM((n, reqs, HD), jnp.bfloat16),
            pltpu.VMEM((blocks, merged, block), jnp.bfloat16),
            pltpu.VMEM((blocks, merged, block), jnp.bfloat16),
            dma((3,)),
            dma((back // 2, groups, 2)),
            dma((back // 2, groups, 2)),
            dma((back // 2, groups, 2)),
            dma((back // 2, groups, 2)),
            dma((heads,)),
            dma((n,)),
            dma((n - 1,)),
            dma((n,)),
            dma((blocks,)),
            dma((blocks,)),
        ],
        compiler_params=pltpu.CompilerParams(
            collective_id=0, has_side_effects=True, vmem_limit_bytes=60 * 1024 * 1024
        ),
    )(
        prefill_query, prefill_key, prefill_value, lo, col_req, dec_query, dec_key, dec_value,
        cache_key, cache_value, out_proj,
    )


def solution(mesh):
    placed = (
        P(("rep", "seq"), "tp"),
        P(("rep", "seq"), "tp"),
        P(("rep", "seq"), "tp"),
        P("rep"),
        P("tp"),
        P("rep", "tp"),
        P("rep", "tp"),
        P("rep", "tp"),
        P(("rep", "seq"), "tp"),
        P(("rep", "seq"), "tp"),
        P(("rep", "seq")),
        P("rep"),
        P("tp", None),
    )
    return jax.shard_map(
        functools.partial(on_device, mesh.shape["seq"]),
        mesh=mesh,
        in_specs=placed,
        out_specs=(P(("rep", "seq", "tp"), None), P(("rep", "tp"), None)),
        check_vma=False,
    )
```

```python
import functools
import math

import jax
import jax.numpy as jnp
from jax import lax
from jax.experimental import pallas as pl
from jax.experimental.pallas import tpu as pltpu
from jax.sharding import PartitionSpec as P

HD = 128
WINDOW = 4096
PAGE = 128
DOCS = 4
MASKED = -1e30
FLOOR = -1e29
MESH = pl.DeviceIdType.MESH


def dot_t(a, b):
    return lax.dot_general(a, b, (((1,), (1,)), ((), ())), preferred_element_type=jnp.float32)


def wide(column, width):
    return jnp.concatenate([column] * (width // column.shape[1]), axis=1)


def kernel(
    n, back, pages_request, q, k, v, docs, windows, order, lengths, dq, dk, dv, ck, cv, w,
    out_p, out_d,
    kv, top, tot, acc, lo, rows, ckv, cvv, wv, part, part_log, gathered, gathered_log, mine, att,
    outgoing, incoming,
    local_sem, zs, zr, ys, yr, ps, pr, fs, fr, ts, tr,
):
    me = lax.axis_index("seq")
    core = lax.axis_index("tp")
    other = 1 - core
    odd = lax.rem(me, 2)
    partner = me + 1 - 2 * odd
    tokens = q.shape[0]
    heads = q.shape[1] // HD
    groups = k.shape[1] // HD
    per = heads // groups
    reqs = dq.shape[0]
    scale = 1.0 / math.sqrt(HD)
    exp_scale = scale * math.log2(math.e)

    loads = [
        pltpu.make_async_copy(ck, ckv, local_sem.at[0]),
        pltpu.make_async_copy(cv, cvv, local_sem.at[1]),
        pltpu.make_async_copy(w, wv, local_sem.at[2]),
    ]
    for load in loads:
        load.start()

    barrier = pltpu.get_barrier_semaphore()

    def greet(d, carry):
        pl.semaphore_signal(
            barrier, inc=1, device_id={"seq": lax.rem(me + d, n)}, device_id_type=MESH
        )
        return carry

    lax.fori_loop(1, n, greet, 0)
    pl.semaphore_signal(barrier, inc=1, device_id={"tp": other}, device_id_type=MESH)
    pl.semaphore_wait(barrier, n)

    position = me * tokens + lax.broadcasted_iota(jnp.int32, (tokens, HD), 0)
    place = position.astype(jnp.float32)
    start = jnp.zeros((tokens, HD), jnp.float32)
    for document in range(1, DOCS):
        before = (docs[...] < document).astype(jnp.float32)
        before = jnp.sum(jnp.sum(before, axis=0, keepdims=True), axis=1, keepdims=True)
        start = jnp.where(before <= place, jnp.maximum(start, before), start)
    lo[...] = start.astype(jnp.int32)

    def source(s, g, i):
        if s == 0:
            return (k, v)[i].at[:, pl.ds(g * HD, HD)]
        return kv.at[s - 1, g, i]

    def along(s, g, i):
        return pltpu.make_async_remote_copy(
            src_ref=source(s, g, i),
            dst_ref=kv.at[s + 1, g, i],
            send_sem=zs.at[s // 2, g, i],
            recv_sem=zr.at[s // 2, g, i],
            device_id={"seq": lax.rem(me + 2, n)},
            device_id_type=MESH,
        )

    def across(s, h, g, i):
        return pltpu.make_async_remote_copy(
            src_ref=source(s, g, i),
            dst_ref=kv.at[2 * h - 2, g, i],
            send_sem=ys.at[h - 1, g, i],
            recv_sem=yr.at[h - 1, g, i],
            device_id={"seq": partner},
            device_id_type=MESH,
        )

    def forward(s, g, finish=False):
        act = (lambda c: c.wait_send()) if finish else (lambda c: c.start())
        if s + 2 <= back:
            @pl.when((me >= s) & (me + 2 < n))
            def _():
                for i in range(2):
                    act(along(s, g, i))

            @pl.when((me >= s) & (odd == 0))
            def _():
                for i in range(2):
                    act(across(s, s // 2 + 1, g, i))
        if s >= 2:
            @pl.when((me >= s) & (odd == 1))
            def _():
                for i in range(2):
                    act(across(s, s // 2, g, i))

    def arrive(s, g):
        @pl.when(me >= s)
        def _():
            for i in range(2):
                if s % 2 == 0:
                    along(s - 2, g, i).wait_recv()
                else:
                    across(s + 1, (s + 1) // 2, g, i).wait_recv()

        if s % 2 == 0:
            forward(s, g)

    def attend(s, g):
        def one_head(r, carry):
            head = g * per + r
            queries = q[:, pl.ds(pl.multiple_of(head * HD, HD), HD)]
            if s == 0:
                keys = k[:, g * HD:(g + 1) * HD]
                values = v[:, g * HD:(g + 1) * HD]
            else:
                keys = kv[s - 1, g, 0]
                values = kv[s - 1, g, 1]
            scores = dot_t(queries, keys)
            column = lax.broadcasted_iota(jnp.int32, (tokens, tokens), 1)
            place = me * tokens + lax.broadcasted_iota(jnp.int32, (tokens, HD), 0)
            limit = jnp.maximum(lo[...], place - windows[head] + 1) - (me - s) * tokens
            allowed = column >= wide(limit, tokens)
            if s == 0:
                allowed = allowed & (
                    column <= lax.broadcasted_iota(jnp.int32, (tokens, tokens), 0)
                )
            scores = jnp.where(allowed, scores, MASKED)
            high = jnp.max(scores, axis=1, keepdims=True) * exp_scale
            high = jnp.broadcast_to(high, (tokens, HD))
            if s > 0:
                old = top[head]
                high = jnp.maximum(high, old)
            weights = jnp.exp2(scores * exp_scale - wide(high, tokens))
            total = jnp.broadcast_to(jnp.sum(weights, axis=1, keepdims=True), (tokens, HD))
            added = jnp.dot(
                weights.astype(jnp.bfloat16), values, preferred_element_type=jnp.float32
            )
            if s > 0:
                shrink = jnp.exp2(old - high)
                total = total + tot[head] * shrink
                added = added + acc[head] * shrink
            top[head] = high
            tot[head] = total
            acc[head] = added
            return carry

        @pl.when(me >= s)
        def _():
            lax.fori_loop(0, per, one_head, 0)

    def to_owner(head):
        return [
            pltpu.make_async_remote_copy(
                src_ref=src.at[head],
                dst_ref=dst.at[me],
                send_sem=ps.at[head, i],
                recv_sem=pr.at[me, i],
                device_id={"seq": head},
                device_id_type=MESH,
            )
            for i, (src, dst) in enumerate(((part, gathered), (part_log, gathered_log)))
        ]

    def decode_partials():
        loads[0].wait()
        loads[1].wait()
        pages = order.shape[0]
        step = math.gcd(pages, 8)
        row_req = jnp.concatenate(
            [lax.broadcasted_iota(jnp.int32, (reqs, step * PAGE), 0)] * per, axis=0
        )
        for g in range(groups):
            queries = jnp.concatenate(
                [dq[:, (g * per + r) * HD:(g * per + r + 1) * HD] for r in range(per)], axis=0
            )

            def block(b, carry):
                high_old, total_old, acc_old = carry
                span = pl.ds(pl.multiple_of(b * step * PAGE, step * PAGE), step * PAGE)
                keys = ckv[span, g * HD:(g + 1) * HD]
                values = cvv[span, g * HD:(g + 1) * HD]
                lane = lax.broadcasted_iota(jnp.int32, (1, PAGE), 1)
                reqs_of = []
                for i in range(step):
                    page = order[b * step + i]
                    owner = page // pages_request
                    left = lengths[owner] - (page - owner * pages_request) * PAGE
                    reqs_of.append(jnp.where(lane < left, owner, -1))
                reqs_of = jnp.concatenate(reqs_of, axis=1)
                scores = jnp.where(row_req == reqs_of, dot_t(queries, keys), MASKED)
                high = jnp.max(scores, axis=1, keepdims=True)
                high = jnp.maximum(high, FLOOR) * exp_scale
                high = jnp.maximum(jnp.broadcast_to(high, (per * reqs, HD)), high_old)
                weights = jnp.exp2(scores * exp_scale - wide(high, step * PAGE))
                total = jnp.sum(weights, axis=1, keepdims=True)
                shrink = jnp.exp2(high_old - high)
                added = jnp.dot(
                    weights.astype(jnp.bfloat16), values, preferred_element_type=jnp.float32
                )
                return (high, total + total_old * shrink, added + acc_old * shrink)

            zero = jnp.zeros((per * reqs, HD), jnp.float32)
            high, total, added = lax.fori_loop(
                0, pages // step, block, (zero + FLOOR * exp_scale, zero, zero)
            )
            for r in range(per):
                cut = slice(r * reqs, (r + 1) * reqs)
                some = total[cut] > 0.0
                whole = jnp.where(some, total[cut], 1.0)
                part[g * per + r] = (added[cut] / whole).astype(jnp.bfloat16)
                level = jnp.where(some, high[cut] + jnp.log2(whole), FLOOR)
                if reqs < HD:
                    level = jnp.concatenate(
                        [level, jnp.zeros((HD - reqs, HD), jnp.float32)], axis=0
                    )
                part_log[g * per + r] = level.T[:8]
        for head in range(heads):
            @pl.when(me != head)
            def _():
                for copy in to_owner(head):
                    copy.start()

    def from_owner(d):
        return pltpu.make_async_remote_copy(
            src_ref=mine,
            dst_ref=att.at[me],
            send_sem=fs.at[d - 1],
            recv_sem=fr.at[me],
            device_id={"seq": lax.rem(me + d, n)},
            device_id_type=MESH,
        )

    def wait_partial(j):
        for i, (src, dst) in enumerate(((part, gathered), (part_log, gathered_log))):
            pltpu.make_async_remote_copy(
                src_ref=src.at[0],
                dst_ref=dst.at[j],
                send_sem=ps.at[0, i],
                recv_sem=pr.at[j, i],
                device_id={"seq": partner},
                device_id_type=MESH,
            ).wait_recv()

    def wait_final(head):
        return pltpu.make_async_remote_copy(
            src_ref=mine,
            dst_ref=att.at[head],
            send_sem=fs.at[0],
            recv_sem=fr.at[head],
            device_id={"seq": partner},
            device_id_type=MESH,
        )

    def decode_merge():
        @pl.when(me < heads)
        def _():
            head = me
            queries = dq[:, pl.ds(pl.multiple_of(head * HD, HD), HD)].astype(jnp.float32)
            group = pl.ds(pl.multiple_of((head // per) * HD, HD), HD)
            own = jnp.sum(queries * dk[:, group].astype(jnp.float32), axis=1, keepdims=True)
            own = jnp.broadcast_to(own * exp_scale, (reqs, HD))
            value = dv[:, group].astype(jnp.float32)

            def join(carry, logs, parts):
                high_old, total_old, sum_old = carry
                level = jnp.broadcast_to(logs[:1], (HD, HD)).T[:reqs]
                fresh = jnp.maximum(high_old, level)
                left = jnp.exp2(high_old - fresh)
                right = jnp.exp2(level - fresh)
                return (
                    fresh,
                    total_old * left + right,
                    sum_old * left + parts.astype(jnp.float32) * right,
                )

            def take(d, carry):
                j = lax.rem(me + d, n)
                wait_partial(j)
                return join(carry, gathered_log[j], gathered[j])

            carry = join((own, jnp.ones_like(own), value), part_log[head], part[head])
            high, total, summed = lax.fori_loop(1, n, take, carry)
            final = (summed / total).astype(jnp.bfloat16)
            mine[...] = final

            def send(d, carry):
                from_owner(d).start()
                return carry

            lax.fori_loop(1, n, send, 0)

    for g in range(groups):
        forward(0, g)
    for g in range(groups):
        attend(0, g)
    arrive(2, 0)
    decode_partials()
    for g in range(1, groups):
        arrive(2, g)
    for g in range(groups):
        attend(2, g)
    for h in range(1, back // 2 + 1):
        for g in range(groups):
            if 2 * h + 2 <= back:
                arrive(2 * h + 2, g)
            arrive(2 * h - 1, g)
            attend(2 * h - 1, g)
        if h == 1:
            decode_merge()
        if 2 * h + 2 <= back:
            for g in range(groups):
                attend(2 * h + 2, g)

    half = tokens // 2
    half_reqs = reqs // 2
    for head in range(heads):
        cut = slice(head * HD, (head + 1) * HD)
        done = (acc[head] / tot[head]).astype(jnp.bfloat16)
        for c in range(2):
            rows[c, :half, cut] = done[c * half:(c + 1) * half]

        @pl.when(me == head)
        def _():
            for c in range(2):
                rows[c, half:, cut] = mine[c * half_reqs:(c + 1) * half_reqs]

        @pl.when(me != head)
        def _():
            wait_final(head).wait_recv()
            for c in range(2):
                rows[c, half:, cut] = att[head, c * half_reqs:(c + 1) * half_reqs]

    loads[2].wait()
    blocks = outgoing.shape[0]
    width = outgoing.shape[2]

    def exchange(b):
        return pltpu.make_async_remote_copy(
            src_ref=outgoing.at[b],
            dst_ref=incoming.at[b],
            send_sem=ts.at[b],
            recv_sem=tr.at[b],
            device_id={"tp": other},
            device_id_type=MESH,
        )

    def project(c, b):
        span = pl.ds(pl.multiple_of(b * width, width), width)
        return jnp.dot(rows[c], wv[:, span], preferred_element_type=jnp.float32)

    def give(b, carry):
        outgoing[b] = project(other, b).astype(jnp.bfloat16)
        exchange(b).start()
        return carry

    def keep(b, carry):
        own = project(core, b).astype(jnp.bfloat16).astype(jnp.float32)
        exchange(b).wait_recv()
        total = (own + incoming[b].astype(jnp.float32)).astype(jnp.bfloat16)
        span = pl.ds(pl.multiple_of(b * width, width), width)
        out_p[:, span] = total[:half]
        out_d[:, span] = total[half:]
        return carry

    lax.fori_loop(0, blocks, give, 0)
    lax.fori_loop(0, blocks, keep, 0)

    def sent(b, carry):
        exchange(b).wait_send()
        return carry

    lax.fori_loop(0, blocks, sent, 0)
    for s in range(0, back + 1, 2):
        for g in range(groups):
            forward(s, g, finish=True)
    for head in range(heads):
        @pl.when(me != head)
        def _():
            for copy in to_owner(head):
                copy.wait_send()

    @pl.when(me < heads)
    def _():
        def sent_final(d, carry):
            from_owner(d).wait_send()
            return carry

        lax.fori_loop(1, n, sent_final, 0)


def on_device(
    n, prefill_query, prefill_key, prefill_value, doc_ids, head_window, dec_query, dec_key,
    dec_value, cache_key, cache_value, page_order, lengths, out_proj,
):
    tokens, width = prefill_query.shape
    heads = width // HD
    groups = prefill_key.shape[1] // HD
    reqs = dec_query.shape[0]
    model = out_proj.shape[1]
    pages = page_order.shape[0]
    reach = min(doc_ids.shape[0] // 2, WINDOW)
    back = -(-reach // tokens)
    back += back % 2

    pages_request = page_order.shape[0] * n // reqs
    docs = doc_ids.reshape(-1, HD)
    vmem = pl.BlockSpec(memory_space=pltpu.VMEM)
    hbm = pl.BlockSpec(memory_space=pl.ANY)
    smem = pl.BlockSpec(memory_space=pltpu.SMEM)
    block = 512
    blocks = model // block
    merged = (tokens + reqs) // 2
    dma = pltpu.SemaphoreType.DMA
    return pl.pallas_call(
        functools.partial(kernel, n, back, pages_request),
        out_shape=(
            jax.ShapeDtypeStruct((tokens // 2, model), jnp.bfloat16),
            jax.ShapeDtypeStruct((reqs // 2, model), jnp.bfloat16),
        ),
        in_specs=[vmem] * 4 + [smem] * 3 + [vmem] * 3 + [hbm] * 3,
        out_specs=(vmem, vmem),
        scratch_shapes=[
            pltpu.VMEM((back, groups, 2, tokens, HD), jnp.bfloat16),
            pltpu.VMEM((heads, tokens, HD), jnp.float32),
            pltpu.VMEM((heads, tokens, HD), jnp.float32),
            pltpu.VMEM((heads, tokens, HD), jnp.float32),
            pltpu.VMEM((tokens, HD), jnp.int32),
            pltpu.VMEM((2, merged, heads * HD), jnp.bfloat16),
            pltpu.VMEM(cache_key.shape, jnp.bfloat16),
            pltpu.VMEM(cache_value.shape, jnp.bfloat16),
            pltpu.VMEM(out_proj.shape, jnp.bfloat16),
            pltpu.VMEM((heads, reqs, HD), jnp.bfloat16),
            pltpu.VMEM((heads, 8, HD), jnp.float32),
            pltpu.VMEM((n, reqs, HD), jnp.bfloat16),
            pltpu.VMEM((n, 8, HD), jnp.float32),
            pltpu.VMEM((reqs, HD), jnp.bfloat16),
            pltpu.VMEM((n, reqs, HD), jnp.bfloat16),
            pltpu.VMEM((blocks, merged, block), jnp.bfloat16),
            pltpu.VMEM((blocks, merged, block), jnp.bfloat16),
            dma((3,)),
            dma((back // 2, groups, 2)),
            dma((back // 2, groups, 2)),
            dma((back // 2, groups, 2)),
            dma((back // 2, groups, 2)),
            dma((heads, 2)),
            dma((n, 2)),
            dma((n - 1,)),
            dma((n,)),
            dma((blocks,)),
            dma((blocks,)),
        ],
        compiler_params=pltpu.CompilerParams(
            collective_id=0, has_side_effects=True, vmem_limit_bytes=60 * 1024 * 1024
        ),
    )(
        prefill_query, prefill_key, prefill_value, docs, head_window, page_order, lengths,
        dec_query, dec_key, dec_value, cache_key, cache_value, out_proj,
    )


def solution(mesh):
    placed = (
        P(("rep", "seq"), "tp"),
        P(("rep", "seq"), "tp"),
        P(("rep", "seq"), "tp"),
        P("rep"),
        P("tp"),
        P("rep", "tp"),
        P("rep", "tp"),
        P("rep", "tp"),
        P(("rep", "seq"), "tp"),
        P(("rep", "seq"), "tp"),
        P(("rep", "seq")),
        P("rep"),
        P("tp", None),
    )
    return jax.shard_map(
        functools.partial(on_device, mesh.shape["seq"]),
        mesh=mesh,
        in_specs=placed,
        out_specs=(P(("rep", "seq", "tp"), None), P(("rep", "tp"), None)),
        check_vma=False,
    )
```
